32 devices in a mesh: rows: 8 (over z, y), cols: 4 (over x, core).
Axes of the slice: x: 2, y: 2, z: 4, core: 2. Of those that a mesh axis runs over, the one named last changes fastest.
Arguments:
- weight_up: bfloat16 [12288, 49152], P('rows', 'cols'), may hold values from -0.078125 to 0.078125
- low_up: bfloat16 [12288, 64], P('rows'), may hold values from -0.0546875 to 0.0546875
- high_up: bfloat16 [64, 49152], P(None, 'cols'), may hold values from -0.75 to 0.75
- norm_train: float32 [12288], P(('rows', 'cols')), may hold values from 0.25 to 1.75
- norm_step: float32 [12288], P(('rows', 'cols')), may hold values from -0.3 to 0.3
Outputs:
- serve_up: bfloat16 [12288, 49152], P(None, ('cols', 'rows'))
- scale_up: float32 [49152], P(('cols', 'rows'))
- serve_norm: bfloat16 [12288], replicated
The draws below stay inside these ranges and needn't reach their ends.
All inputs are finite; a program needn't handle non-finite values.
Results may differ from the reference program's by a relative error of at most 0.0004.
Values may be sent and summed in bfloat16 or wider, within the bound.
No kernel may reach another device: no remote copies, remote signals or barrier semaphores. Data moves between devices by JAX's collectives and lax.ppermute only.
A program may use at most 256 MiB of HBM per device.

```python
import jax
import jax.numpy as jnp
from jax import lax

D_MODEL = 12288
D_INNER = 49152
RANK = 64


def raised(array, own_key, source, target, parts, factor):
    owner, partner = [(jnp.arange(array.shape[position]) // (array.shape[position] // parts)).reshape([-1 if axis == position else 1 for axis in range(array.ndim)]) for position in (source, target)]
    chosen = jax.random.permutation(own_key, parts)[partner]
    strong = (owner == chosen) | (owner == (partner + parts // 2) % parts)
    return jnp.where(strong, factor * array, array)


def shard_levels(own_key, shape, cuts, smallest, largest):
    level = 1.0
    for position, shards_of in cuts:
        draws = jax.random.uniform(jax.random.fold_in(jax.random.fold_in(own_key, 6), position), (shards_of,), jnp.float32, smallest / len(cuts), largest / len(cuts))
        level = level * jnp.repeat(jnp.exp(draws), shape[position] // shards_of).reshape((-1,) + (1,) * (len(shape) - 1 - position))
    return level


def gaussian(own_key, dims, width, limit, cuts=(), held_as=jnp.bfloat16):
    array = jax.random.normal(own_key, dims, jnp.float32) * width
    if len(cuts) > 0:
        array = shard_levels(own_key, dims, cuts, -0.22, 0.18) * array
    return jnp.clip(array, min=-limit, max=limit).astype(held_as)


def heavy_noise(key, dims, deviation, reach, shards, heavy, held_as=jnp.bfloat16):
    entries = deviation * jax.random.normal(key, dims, jnp.float32)
    if shards:
        entries = entries * shard_levels(key, dims, shards, -0.22, 0.18)
    return jnp.clip(raised(entries, jax.random.fold_in(key, 3), *heavy), -reach, reach).astype(held_as)


def setup_inputs(seed: int = 0) -> dict:
    key_of = jax.random.split(jax.random.key(seed), 6)
    return {
        "weight_up": heavy_noise(key_of[0], (D_MODEL, D_INNER), D_MODEL ** -0.5, 0.078125, ((0, 8), (1, 4)), (0, 1, 8, 2.0)),
        "low_up": gaussian(key_of[1], (D_MODEL, RANK), D_MODEL ** -0.5, 0.0546875, ((0, 8),)),
        "high_up": gaussian(key_of[2], (RANK, D_INNER), RANK ** -0.5, 0.75, ((1, 4),)),
        "norm_train": jnp.clip(1.0 + 0.15 * jax.random.normal(key_of[3], (D_MODEL,), jnp.float32), 0.25, 1.75),
        "norm_step": jnp.clip(jax.random.uniform(key_of[4], (D_MODEL,), jnp.float32, -0.3, 0.3) * shard_levels(key_of[4], (D_MODEL,), ((0, 32),), -0.4, 0.0), -0.3, 0.3),
    }


mix_rate = 0.5

def reference(weight_up, low_up, high_up, norm_train, norm_step):
    fresh_up = weight_up.astype(jnp.float32) + mix_rate * jnp.dot(low_up, high_up, preferred_element_type=jnp.float32)
    scale_up = jnp.sqrt(lax.optimization_barrier(jnp.sum(fresh_up * fresh_up, axis=0)))
    serve_up = (fresh_up / scale_up).astype(jnp.bfloat16)
    serve_norm = (norm_train + norm_step).astype(jnp.bfloat16)
    return (serve_up, scale_up, serve_norm)
```

```python
import functools
import math

import jax
import jax.numpy as jnp
from jax import lax
from jax.experimental import pallas as pl
from jax.experimental.pallas import tpu as pltpu
from jax.sharding import PartitionSpec as P


mix_rate = 0.5
lanes = 128
row_pack = 16


def chunk_widths(width):
    if width % lanes or width < 4 * lanes:
        return (width,)
    return (lanes, width - 2 * lanes, lanes)


def pack_kernel(weight_ref, *refs):
    chunk_ref = refs[-1]
    rows = weight_ref.shape[0]
    chunk_ref[0, :rows, :] = weight_ref[...]
    if len(refs) == 2:
        chunk_ref[0, rows:, :] = refs[0][...]


def pack(weight, rider, parts, start, part, width):
    rows = weight.shape[0]
    if part % lanes or width % lanes:
        chunk = jnp.transpose(
            weight.reshape(rows, parts, width)[:, :, start : start + part], (1, 0, 2)
        )
        if rider is not None:
            riders = jnp.broadcast_to(rider[None], (parts,) + rider.shape)
            chunk = jnp.concatenate([chunk, riders], axis=1)
        return chunk
    tile = math.gcd(math.gcd(width, start), part)
    tall = rows + (0 if rider is None else rider.shape[0])
    in_specs = [pl.BlockSpec((rows, tile), lambda d, j: (0, (d * width + start) // tile + j))]
    operands = [weight]
    if rider is not None:
        in_specs.append(pl.BlockSpec((rider.shape[0], tile), lambda d, j: (0, j)))
        operands.append(rider)
    return pl.pallas_call(
        pack_kernel,
        grid=(parts, part // tile),
        in_specs=in_specs,
        out_specs=pl.BlockSpec((1, tall, tile), lambda d, j: (d, 0, j)),
        out_shape=jax.ShapeDtypeStruct((parts, tall, part), weight.dtype),
        compiler_params=pltpu.CompilerParams(
            dimension_semantics=("arbitrary", "arbitrary"),
            vmem_limit_bytes=24 * 1024 * 1024,
        ),
        name="pack",
    )(*operands)


def normalise_kernel(rows, sub, w_ref, low_ref, high_ref, *refs):
    serve_ref, scale_ref, fresh_ref, sum_ref = refs[-4:]
    phase = pl.program_id(1)
    step = pl.program_id(2)
    group = w_ref.shape[0]
    width = w_ref.shape[2]
    fold = sum_ref.shape[0]
    streamed = low_ref.shape[0] < fresh_ref.shape[0]

    @pl.when(phase == 0)
    def _():
        @pl.when(step == 0)
        def _():
            sum_ref[...] = jnp.zeros_like(sum_ref)

        high = high_ref[...]

        def one(g, total):
            base = (step * group + g) * rows
            for s in range(0, rows, sub):
                at = pl.ds(pl.multiple_of(base + s, row_pack), sub)
                low = low_ref[pl.ds(pl.multiple_of(g * rows + s, row_pack), sub), :] if streamed else low_ref[at, :]
                mixed = jnp.dot(low, high, preferred_element_type=jnp.float32)
                fresh = w_ref[g, pl.ds(s, sub), :].astype(jnp.float32) + mixed
                fresh_ref[at, :] = fresh
                total = total + jnp.sum((fresh * fresh).reshape(sub // fold, fold, width), axis=0)
            return total

        sum_ref[...] = lax.fori_loop(0, group, one, sum_ref[...])

    @pl.when(phase == 1)
    def _():
        @pl.when(step == 0)
        def _():
            scale = jnp.sqrt(jnp.sum(sum_ref[...], axis=0, keepdims=True))
            scale_ref[...] = scale
            sum_ref[...] = jnp.broadcast_to(1.0 / scale, sum_ref.shape)

        inverse = sum_ref[0:1, :]

        def one(g, carry):
            base = g * rows
            for s in range(0, rows, sub):
                there = pl.ds(pl.multiple_of(base + s, row_pack), sub)
                here = pl.ds(pl.multiple_of(step * group * rows + base + s, row_pack), sub)
                serve_ref[there, :] = (fresh_ref[here, :] * inverse).astype(jnp.bfloat16)
            return carry

        lax.fori_loop(0, group, one, 0)


def normalise(arrived, low_all, high, serve, rows, start, serve_shape):
    parts, _, width = arrived.shape
    tile = next(t for t in (256, 128, width) if width % t == 0 and start % t == 0)
    base = start // tile
    whole = serve_shape[0]
    steps = 4 if parts % 4 == 0 else 1
    group = parts // steps
    sub = next(s for s in (256, 128, 64, 32, 16) if rows % s == 0)
    fold = 32 if sub % 32 == 0 else 8
    if width == tile:
        low_spec = pl.BlockSpec(
            (group * rows, low_all.shape[1]), lambda j, p, i: (jnp.where(p == 0, i, steps - 1), 0)
        )
    else:
        low_spec = pl.BlockSpec((whole, low_all.shape[1]), lambda j, p, i: (0, 0))
    in_specs = [
        pl.BlockSpec((group, rows, tile), lambda j, p, i: (jnp.where(p == 0, i, steps - 1), 0, j)),
        low_spec,
        pl.BlockSpec((high.shape[0], tile), lambda j, p, i: (0, j)),
    ]
    operands = [arrived, low_all, high]
    aliases = {}
    if serve is not None:
        in_specs.append(pl.BlockSpec(memory_space=pl.ANY))
        operands.append(serve)
        aliases = {3: 0}
    return pl.pallas_call(
        functools.partial(normalise_kernel, rows, sub),
        grid=(width // tile, 2, steps),
        in_specs=in_specs,
        out_specs=[
            pl.BlockSpec((group * rows, tile), lambda j, p, i: (jnp.where(p == 0, 0, i), base + j)),
            pl.BlockSpec((1, tile), lambda j, p, i: (0, j)),
        ],
        out_shape=[
            jax.ShapeDtypeStruct(serve_shape, jnp.bfloat16),
            jax.ShapeDtypeStruct((1, width), jnp.float32),
        ],
        scratch_shapes=[
            pltpu.VMEM((whole, tile), jnp.float32),
            pltpu.VMEM((fold, tile), jnp.float32),
        ],
        input_output_aliases=aliases,
        compiler_params=pltpu.CompilerParams(
            dimension_semantics=("arbitrary", "arbitrary", "arbitrary"),
            vmem_limit_bytes=48 * 1024 * 1024,
        ),
        name="normalise",
    )(*operands)


def per_device(n_rows, n_cols, weight_up, low_up, high_up, norm_train, norm_step):
    rows, span = weight_up.shape
    rank = low_up.shape[1]
    width = span // n_rows
    piece = rows // n_cols
    whole = rows * n_rows
    row_place = lax.axis_index("rows")
    col_place = lax.axis_index("cols")
    widths = chunk_widths(width)

    norm = (norm_train + norm_step).astype(jnp.bfloat16)
    low_turned = lax.dynamic_slice_in_dim(low_up.T, col_place * piece, piece, axis=1)
    rider = jnp.concatenate([low_turned, norm[None]], axis=0)
    held = rider.size
    unit = row_pack * widths[0]
    rider = jnp.pad(rider.reshape(-1), (0, -held % unit)).reshape(-1, widths[0])

    arrivals = []
    start = 0
    for index, part in enumerate(widths):
        chunk = pack(weight_up, None if index else rider, n_rows, start, part, width)
        arrived = lax.all_to_all(chunk, "rows", split_axis=0, concat_axis=0, tiled=True)
        arrivals.append(arrived)
        start += part

    mine = arrivals[0][:, rows:, :].reshape(n_rows, -1)[:, :held].reshape(n_rows, rank + 1, piece)
    spread = jnp.zeros((n_cols,) + mine.shape, mine.dtype)
    spread = lax.dynamic_update_index_in_dim(spread, mine, col_place, 0)
    for shift in range(1, n_cols):
        came = lax.ppermute(mine, "cols", [(c, (c + shift) % n_cols) for c in range(n_cols)])
        spread = lax.dynamic_update_index_in_dim(spread, came, (col_place - shift) % n_cols, 0)
    low_all = jnp.transpose(spread[:, :, :rank, :], (1, 0, 3, 2)).reshape(whole, rank)
    serve_norm = jnp.transpose(spread[:, :, rank, :], (1, 0, 2)).reshape(whole)

    high_own = mix_rate * lax.dynamic_slice_in_dim(high_up, row_place * width, width, axis=1)
    serve = None
    scales = []
    start = 0
    for part, arrived in zip(widths, arrivals):
        serve, scale = normalise(
            arrived, low_all, high_own[:, start : start + part], serve, rows, start, (whole, width)
        )
        scales.append(scale[0])
        start += part
    return (serve, jnp.concatenate(scales), serve_norm)


def in_layer(n_rows, n_cols, *args):
    return per_device(n_rows, n_cols, *args)


def solution(mesh):
    in_specs = (
        P("rows", "cols"),
        P("rows", None),
        P(None, "cols"),
        P(("rows", "cols")),
        P(("rows", "cols")),
    )
    out_specs = (P(None, ("cols", "rows")), P(("cols", "rows")), P())
    body = functools.partial(in_layer, mesh.shape["rows"], mesh.shape["cols"])
    return jax.shard_map(body, mesh=mesh, in_specs=in_specs, out_specs=out_specs, check_vma=False)
```
